768 devices in a mesh: srv: 48 (over z, y_lo), blk: 8 (over x, y_hi), rep: 2 (over core).
Axes of the slice: x: 4, y: 8 (y_hi: 2, y_lo: 4; y = y_hi * 4 + y_lo), z: 12, core: 2. Of those that a mesh axis runs over, the one named last changes fastest.
Arguments:
- queries: bfloat16 [48, 8, 256, 4096], P('srv', 'blk', 'rep'), parts along dimension 2, may hold values from -16 to 16
- destination: int32 [48, 8, 64], P('srv', 'blk', 'rep'), parts along dimension 2, may hold values from 0 to 47, as said below
- offsets: int32 [48, 8, 64], P('srv', 'blk', 'rep'), parts along dimension 2, may hold values from 0 to 124
- key_rows: bfloat16 [48, 1024, 512], P('srv', 'blk', 'rep'), parts along dimension 2, may hold values from -16 to 16
- value_rows: bfloat16 [48, 1024, 512], P('srv', 'blk', 'rep'), parts along dimension 2, may hold values from -6 to 6
- lengths: int32 [48, 16], P('srv', 'rep'), parts along dimension 1, may hold values from 1 to 385, 1024 in all within a row
Outputs:
- attended: bfloat16 [48, 8, 256, 4096], P('srv', 'blk', 'rep'), parts along dimension 2
The draws below stay inside these ranges and needn't reach their ends.
There are 2 independent parts, one for each index of `rep`. The reference program is written for one: setup_inputs(seed, part) draws one part's arguments, and reference() takes and returns one part's arrays. A program takes and returns all parts, laid end to end along the dimension named above; each array names one. Nothing has to cross between parts.
Inputs may be any that keep to these rules, and one draw needn't show every extreme that they name: `destination`: within each round (tasks r * 16 to r * 16 + 15 of a device) a device names 16 different servers; in each round and for each blk index, 2 servers are named by every device of that blk index.
All inputs are finite; a program needn't handle non-finite values.
Results may differ from the reference program's by a relative error of at most 0.0033.
Values may be sent and summed in bfloat16 or wider, within the bound.
No kernel may reach another device: no remote copies, remote signals or barrier semaphores. Data moves between devices by JAX's collectives and lax.ppermute only.
A program may use at most 32 MiB of HBM per device.

```python
import math
import jax
import jax.numpy as jnp
import numpy as np
from jax import lax

QH = 32
KVH = 2
HD = 128
KVB = 128
R = 4
ROUNDS = 2
HOT = 2
DOCS = 8
TASKS = 16
CTX = 1024
N_SRV = 48
N_BLK = 8


def server_order(subkey):
    return jax.random.permutation(subkey, N_SRV)


def task_order(subkey):
    return jax.random.permutation(subkey, TASKS)


def draw_queries(key, part):
    shape = (N_SRV, N_BLK, ROUNDS * TASKS * R, QH * HD)
    base = jnp.clip(jax.random.normal(jax.random.fold_in(key, 11), shape, jnp.float32), -6.0, 6.0)
    return base.astype(jnp.bfloat16)


def draw_key_rows(key, part):
    shape = (N_SRV, CTX, KVH * HD)
    base = jnp.clip(jax.random.normal(jax.random.fold_in(key, 31), shape, jnp.float32), -6.0, 6.0)
    return base.astype(jnp.bfloat16)


def draw_destination(key, part):
    hot_keys = jax.random.split(jax.random.fold_in(key, 21), N_BLK * ROUNDS)
    hot_list = jax.vmap(server_order)(hot_keys)[:, :HOT]
    everyone = jnp.arange(N_SRV, dtype=jnp.int32)
    is_hot = jnp.any(hot_list[:, :, None] == everyone[None, None, :], axis=1).astype(jnp.int32)
    is_hot = is_hot.reshape(N_BLK, ROUNDS, N_SRV)
    rank_keys = jax.random.split(jax.random.fold_in(key, 22), N_SRV * N_BLK * ROUNDS)
    ranks = jax.vmap(server_order)(rank_keys).reshape(N_SRV, N_BLK, ROUNDS, N_SRV).astype(jnp.int32)
    scores = ranks + N_SRV * is_hot[None]
    picked = lax.top_k(scores, TASKS)[1]
    shuffle_keys = jax.random.split(jax.random.fold_in(key, 23), N_SRV * N_BLK * ROUNDS)
    shuffle = jax.vmap(task_order)(shuffle_keys).reshape(N_SRV, N_BLK, ROUNDS, TASKS)
    picked = jnp.take_along_axis(picked, shuffle, axis=3)
    return picked.reshape(N_SRV, N_BLK, ROUNDS * TASKS).astype(jnp.int32)


def touch_ends(values, stream_key, low, largest):
    place = [jax.random.randint(jax.random.fold_in(stream_key, axis), (), 0, length) for axis, length in enumerate(values.shape)]
    widest = values.shape.index(max(values.shape))
    beside = place[:widest] + [(place[widest] + 1) % values.shape[widest]] + place[widest + 1:]
    return values.at[tuple(place)].set(low).at[tuple(beside)].set(largest)


def levels(stream_key, extent, pieces, smallest, top_value):
    loudness = 1.0
    for dim, shards_of in pieces:
        heights = jax.random.uniform(jax.random.fold_in(jax.random.fold_in(stream_key, 6), dim), (shards_of,), jnp.float32, smallest / len(pieces), top_value / len(pieces))
        loudness = loudness * jnp.repeat(jnp.exp(heights), extent[dim] // shards_of).reshape((-1,) + (1,) * (len(extent) - 1 - dim))
    return loudness


def split_up(amount, total, most, slope):
    portions = [(1 << 20) // math.isqrt(grade ** slope) + 1 for grade in range(2, amount + 1)]
    surplus, holding = total - most - (amount - 1), [1] * (amount - 1)
    while surplus > 0:
        candidates = [i for i in range(amount - 1) if holding[i] < most]
        pool, budget = sum([portions[i] for i in candidates]), surplus
        for i in candidates:
            addition = min(most - holding[i], max(1, budget * portions[i] // pool), surplus)
            holding[i] = holding[i] + addition
            surplus = surplus - addition
    return np.array([most] + holding)


def ragged_sizes(stream_key, count, total, most, lean):
    if count == 2:
        one = jax.random.randint(stream_key, (), max(1, total - most), min(most, total - 1) + 1)
        return jnp.stack([one, total - one])
    sizes = jnp.asarray(split_up(count, total, most, lean), jnp.int32)
    twos = (count - 1) // 2
    source_of, taker = sizes[1:1 + 2 * twos:2], sizes[2:2 + 2 * twos:2]
    slack = jnp.minimum(source_of - 1, most - taker)
    passed = jax.random.randint(jax.random.fold_in(stream_key, 1), (twos,), 0, 1 << 20) % (slack + 1)
    sizes = sizes.at[1:1 + 2 * twos:2].set(source_of - passed).at[2:2 + 2 * twos:2].set(taker + passed)
    return sizes[jax.random.permutation(jax.random.fold_in(stream_key, 2), count)]


def centred(key, extent, scale, most, shards=(), kind=jnp.bfloat16):
    gain = levels(key, extent, shards, -0.22, 0.18) if shards else 1.0
    entries = jax.random.normal(key, extent, jnp.float32) * scale * gain
    return jnp.minimum(jnp.maximum(entries, -most), most).astype(kind)


def setup_inputs(seed: int = 0, part: int = 0) -> dict:
    seeds = jax.random.split(jax.random.key(seed), 7)
    part_splits = jax.random.split(jax.random.fold_in(seeds[6], part), 7)
    queries = draw_queries(jax.random.fold_in(jax.random.fold_in(seeds[6], part), 71), part)
    destination = draw_destination(jax.random.fold_in(jax.random.fold_in(seeds[6], part), 71), part)
    offsets = touch_ends(jax.random.randint(part_splits[2], (N_SRV, N_BLK, ROUNDS * TASKS), 0, KVB - R + 1), jax.random.fold_in(part_splits[2], 1), 0, KVB - R).astype(jnp.int32)
    key_rows = draw_key_rows(jax.random.fold_in(jax.random.fold_in(seeds[6], part), 71), part)
    value_rows = centred(part_splits[4], (N_SRV, CTX, KVH * HD), 1.0, 6.0, ((0, 48), (1, 8)))
    lengths = jax.vmap(lambda own: ragged_sizes(own, DOCS, CTX, 3 * KVB + 1, 1))(jax.random.split(part_splits[5], N_SRV)).reshape((N_SRV, DOCS)).astype(jnp.int32)
    return dict(queries=queries, destination=destination, offsets=offsets, key_rows=key_rows, value_rows=value_rows, lengths=lengths)


def attend_task(query_block, target, start, column, key_rows, value_rows, boundary):
    span = 3 * KVB + R
    groups = QH // KVH
    scaling = 1.0 / math.sqrt(HD)
    target = target.astype(jnp.int32)
    first = (column * KVB + start).astype(jnp.int32)
    anchor = jnp.clip(first - 3 * KVB, 0, CTX - span).astype(jnp.int32)
    zero = jnp.zeros((), jnp.int32)
    key_block = lax.dynamic_slice(key_rows, (target, anchor, zero), (1, span, KVH * HD))[0]
    value_block = lax.dynamic_slice(value_rows, (target, anchor, zero), (1, span, KVH * HD))[0]
    ends = lax.dynamic_slice(boundary, (target, zero), (1, DOCS))[0]
    query_pos = first + jnp.arange(R, dtype=jnp.int32)
    key_pos = anchor + jnp.arange(span, dtype=jnp.int32)
    query_doc = lax.optimization_barrier(jnp.sum((ends[None, :] <= query_pos[:, None]).astype(jnp.int32), axis=1))
    key_doc = lax.optimization_barrier(jnp.sum((ends[None, :] <= key_pos[:, None]).astype(jnp.int32), axis=1))
    allowed = (key_pos[None, :] <= query_pos[:, None]) & (key_doc[None, :] == query_doc[:, None])
    query_heads = query_block.astype(jnp.float32).reshape(R, KVH, groups, HD)
    key_heads = key_block.astype(jnp.float32).reshape(span, KVH, HD)
    value_heads = value_block.astype(jnp.float32).reshape(span, KVH, HD)
    scores = jnp.einsum('rkgd,nkd->kgrn', query_heads, key_heads) * scaling
    scores = jnp.where(allowed[None, None], scores, -1e+30)
    highest = lax.optimization_barrier(jnp.max(scores, axis=3, keepdims=True))
    weights = jnp.exp(scores - highest)
    denominator = lax.optimization_barrier(jnp.sum(weights, axis=3))
    rounded = lax.optimization_barrier(weights.astype(jnp.bfloat16)).astype(jnp.float32)
    weighted = jnp.einsum('kgrn,nkd->rkgd', rounded, value_heads)
    result = weighted / jnp.transpose(denominator, (2, 0, 1))[..., None]
    return result.reshape(R, QH * HD).astype(jnp.bfloat16)

def reference(queries, destination, offsets, key_rows, value_rows, lengths):
    boundary = jnp.cumsum(lengths, axis=1).astype(jnp.int32)
    task_count = ROUNDS * TASKS
    flat_queries = queries.reshape(N_SRV * N_BLK, task_count, R, QH * HD)
    flat_targets = destination.reshape(N_SRV * N_BLK, task_count)
    flat_starts = offsets.reshape(N_SRV * N_BLK, task_count)
    columns = jnp.tile(jnp.arange(N_BLK, dtype=jnp.int32), N_SRV)

    def one_device(bundle):
        query_group, target_group, start_group, column = bundle

        def per_task(query_block, target, start):
            return attend_task(query_block, target, start, column, key_rows, value_rows, boundary)
        return jax.vmap(per_task)(query_group, target_group, start_group)
    answers = lax.map(one_device, (flat_queries, flat_targets, flat_starts, columns))
    return answers.reshape(N_SRV, N_BLK, task_count * R, QH * HD)
```

```python
import math

import jax
import jax.numpy as jnp
from jax import lax
from jax.experimental import pallas as pl
from jax.sharding import Mesh
from jax.sharding import PartitionSpec as P

QH = 32
KVH = 2
HD = 128
R = 4
ROUNDS = 2
COLS = 4
GROUPS = QH // KVH
DOCS = 8
BEHIND = 3
SCALE = math.log2(math.e) / math.sqrt(HD)


def attend_kernel(*refs):
    servers = len(refs) // (3 * COLS + 1)
    windows = refs[2 * COLS * servers : (2 * COLS + 1) * servers]
    for s in range(servers):
        serve(
            refs[COLS * s : COLS * (s + 1)],
            refs[COLS * (servers + s) : COLS * (servers + s + 1)],
            windows[s],
            refs[(2 * COLS + 1) * servers + COLS * s : (2 * COLS + 1) * servers + COLS * (s + 1)],
        )


def serve(query_refs, place_refs, window_ref, out_refs):
    slots = ROUNDS * R
    rows = COLS * slots
    span = window_ref.shape[0] - DOCS
    marks = window_ref[span:, : 2 * HD].astype(jnp.float32)
    starts = marks[:, :HD] * 16.0 + marks[:, HD:]
    place = jnp.concatenate([ref[...].astype(jnp.float32) for ref in place_refs], axis=0)
    place = place + float(BEHIND * HD)
    first = jnp.zeros_like(place)
    for doc in range(DOCS):
        start = jnp.broadcast_to(starts[doc : doc + 1, :], place.shape)
        first = jnp.maximum(first, jnp.where(start <= place, start, 0.0))
    lane = lax.broadcasted_iota(jnp.int32, place.shape, 1).astype(jnp.float32)
    bias = []
    for tile in range(span // HD):
        key_pos = lane + float(tile * HD)
        allowed = (key_pos >= first) & (key_pos <= place)
        bias.append(jnp.where(allowed, 0.0, -1e30))
    bias = jnp.concatenate(bias, axis=1)
    parts = 4
    per_part = GROUPS // parts
    for head in range(KVH):
        keys = window_ref[:span, 2 * head * HD : (2 * head + 1) * HD]
        values = window_ref[:span, (2 * head + 1) * HD : (2 * head + 2) * HD]
        for part in range(parts):
            first_head = head * GROUPS + part * per_part
            heads = range(first_head, first_head + per_part)
            query = jnp.concatenate(
                [
                    ref[:, h * HD : (h + 1) * HD].astype(jnp.float32)
                    for h in heads
                    for ref in query_refs
                ],
                axis=0,
            ).astype(jnp.bfloat16)
            scores = lax.dot_general(
                query, keys, (((1,), (1,)), ((), ())), preferred_element_type=jnp.float32
            )
            weights, inverse = [], []
            for n in range(per_part):
                scaled = scores[n * rows : (n + 1) * rows] * SCALE + bias
                weight = jnp.exp2(scaled - jnp.max(scaled, axis=1, keepdims=True))
                inverse.append(1.0 / jnp.sum(weight, axis=1, keepdims=True))
                weights.append(weight.astype(jnp.bfloat16))
            weighted = lax.dot_general(
                jnp.concatenate(weights, axis=0),
                values,
                (((1,), (0,)), ((), ())),
                preferred_element_type=jnp.float32,
            )
            for n, h in enumerate(heads):
                result = weighted[n * rows : (n + 1) * rows] * inverse[n]
                for c, ref in enumerate(out_refs):
                    ref[:, h * HD : (h + 1) * HD] = result[c * slots : (c + 1) * slots].astype(
                        jnp.bfloat16
                    )


def sources_of(order):
    far = 3 if order % 2 == 0 else 4
    return ((0, order), (1, order), (2, order), (far, order // 2))


def attend(arrived, windows, orders):
    slots = ROUNDS * R
    width = QH * HD
    queries, query_specs, place_specs, out_shape = [], [], [], []
    for order in orders:
        for group, at in sources_of(order):
            queries.append(arrived[group])
            query_specs.append(pl.BlockSpec((slots, width), lambda i, at=at: (at, 0)))
            place_specs.append(pl.BlockSpec((slots, HD), lambda i, at=at: (at, width // HD)))
            out_shape.append(jax.ShapeDtypeStruct((slots, width), jnp.bfloat16))
    window_spec = pl.BlockSpec(windows[0].shape, lambda i: (0, 0))
    return pl.pallas_call(
        attend_kernel,
        grid=(1,),
        in_specs=query_specs + place_specs + [window_spec] * len(windows),
        out_specs=[pl.BlockSpec((slots, width), lambda i: (0, 0))] * len(out_shape),
        out_shape=out_shape,
    )(*queries, *queries, *windows)


def along_z(array, by):
    planes = lax.axis_size("z")
    return lax.ppermute(array, "z", [(i, (i + by) % planes) for i in range(planes)])


def along_y(array, by):
    ring = 2 * COLS
    spot = [(i % COLS) * 2 + i // COLS for i in range(ring)]
    pairs = [(spot[i], spot[(i + by) % ring]) for i in range(ring)]
    return lax.ppermute(array, ("col", "yh"), pairs)


def along_x(array, by):
    peers = lax.axis_size("x")
    return lax.ppermute(array, "x", [(i, i + by) for i in range(peers - by)])


def window_of(key_rows, value_rows, lengths):
    x, upper = lax.axis_index("x"), lax.axis_index("yh")
    key, value = key_rows[0], value_rows[0]
    block = key.shape[0]
    joined = jnp.concatenate([key[:, :HD], value[:, :HD], key[:, HD:], value[:, HD:]], axis=1)
    other = lax.ppermute(joined, "yh", [(0, 1), (1, 0)])
    lower_block = jnp.where(upper == 0, joined, other)
    upper_block = jnp.where(upper == 0, other, joined)
    pair = jnp.concatenate([lower_block, upper_block], axis=0)
    pair_behind = along_x(pair, 1)
    last_behind = along_x(upper_block, 2)
    origin = (2 * x - BEHIND) * block
    lowest = jnp.maximum(0, -origin)
    ends = jnp.cumsum(lengths[0])[:-1] - origin
    starts = jnp.concatenate([lowest[None], jnp.clip(ends, lowest, (BEHIND + 2) * block)])
    high = jnp.broadcast_to((starts // 16)[:, None], (DOCS, HD))
    low = jnp.broadcast_to((starts % 16)[:, None], (DOCS, HD))
    marks = jnp.concatenate([high, low, high, low], axis=1).astype(jnp.bfloat16)
    return jnp.concatenate([last_behind, pair_behind, pair, marks], axis=0)


def pick(select, array):
    return jnp.dot(select, array, preferred_element_type=jnp.float32).astype(jnp.bfloat16)


def on_device(queries, destination, offsets, key_rows, value_rows, lengths):
    planes = lax.axis_size("z")
    column, plane = lax.axis_index("col"), lax.axis_index("z")
    upper = lax.axis_index("yh")
    block = key_rows.shape[1]
    rows = destination.shape[2] * R
    slots = ROUNDS * R
    reach = planes // 2
    window = window_of(key_rows, value_rows, lengths)

    target = jnp.repeat(destination[0, 0], R)
    row = jnp.arange(rows, dtype=jnp.int32)
    ahead = (target // COLS - plane) % planes
    order = jnp.where(ahead <= reach, jnp.maximum(2 * ahead - 1, 0), 2 * (planes - ahead))
    within = (row // (rows // ROUNDS)) * R + row % R
    across = (target % COLS - column) % COLS
    place = upper * block + jnp.repeat(offsets[0, 0], R) + row % R
    place = jnp.broadcast_to(place[:, None], (rows, HD)).astype(jnp.bfloat16)
    payload = jnp.concatenate([queries[0, 0], place], axis=1)
    groups = [
        (across == 0, order, 0),
        (across == 1, order, 1),
        (across == 3, order, -1),
        ((across == 2) & (order % 2 == 0), order // 2, 2),
        ((across == 2) & (order % 2 == 1), order // 2, -2),
    ]
    selects, arrived = [], []
    for number, (chosen, at, by) in enumerate(groups):
        count = (planes if number < 3 else reach) * slots
        slot = jnp.arange(count, dtype=jnp.int32)[:, None]
        select = (((at * slots + within)[None, :] == slot) & chosen[None, :]).astype(jnp.bfloat16)
        selects.append(select)
        sending = pick(select, payload)
        arrived.append(along_y(sending, by) if by else sending)

    served = {}

    def serve_orders(windows, orders):
        outs = attend(arrived, windows, orders)
        for n, number in enumerate(orders):
            for c, (group, at) in enumerate(sources_of(number)):
                served[group, at] = outs[COLS * n + c]

    serve_orders([window], [0])
    ahead_window, behind_window = window, window
    width = window.shape[1] // 2
    gathered = None

    def give_back(orders):
        backs, chosen = [], []
        for number, (_, _, by) in enumerate(groups):
            ats = [at for o in orders for group, at in sources_of(o) if group == number]
            if not ats:
                continue
            outgoing = jnp.concatenate([served[number, at] for at in ats], axis=0)
            back = along_y(outgoing, -by) if by else outgoing
            backs.append(back)
            chosen.append(selects[number][ats[0] * slots : (ats[-1] + 1) * slots])
        return pick(jnp.concatenate(chosen, axis=0).T, jnp.concatenate(backs, axis=0))

    for step in range(1, reach):
        ahead_window = along_z(ahead_window, -1)
        behind_window = along_z(behind_window, 1)
        serve_orders([ahead_window, behind_window], [2 * step - 1, 2 * step])
        if step == reach - 2:
            gathered = give_back(list(range(2 * step + 1)))
    last_left = along_z(ahead_window[:, :width], -1)
    last_right = along_z(behind_window[:, width:], 1)
    last = jnp.concatenate([last_left, last_right], axis=1)
    serve_orders([last], [planes - 1])
    rest = give_back(list(range(0 if gathered is None else 2 * (reach - 2) + 1, planes)))
    return (rest if gathered is None else gathered + rest)[None, None]


def solution(mesh):
    shape = dict(mesh.shape)
    fine = Mesh(
        mesh.devices.reshape(shape["srv"] // COLS, COLS, shape["blk"] // 2, 2, shape["rep"]),
        ("z", "col", "x", "yh", "rep"),
    )
    srv, blk = ("z", "col"), ("x", "yh")
    placed = (
        P(srv, blk, "rep", None),
        P(srv, blk, "rep"),
        P(srv, blk, "rep"),
        P(srv, blk, "rep"),
        P(srv, blk, "rep"),
        P(srv, "rep"),
    )

    return jax.shard_map(
        on_device,
        mesh=fine,
        in_specs=placed,
        out_specs=P(srv, blk, "rep", None),
        check_vma=False,
    )
```

```python
import math

import jax
import jax.numpy as jnp
from jax import lax
from jax.experimental import pallas as pl
from jax.experimental.pallas import tpu as pltpu
from jax.sharding import Mesh
from jax.sharding import PartitionSpec as P

QH = 32
KVH = 2
HD = 128
R = 4
ROUNDS = 2
COLS = 4
GROUPS = QH // KVH
DOCS = 8
BEHIND = 3
PARTS = 1
SCALE = math.log2(math.e) / math.sqrt(HD)


def attend_kernel(base, count, groups_out, aliased, *refs):
    query_refs, place_refs = refs[:5], refs[5:10]
    windows = refs[10 : 10 + count]
    out_refs = refs[10 + count + aliased : 10 + count + aliased + len(groups_out)]
    held, far, sems = refs[10 + count + aliased + len(groups_out) :]
    at = pl.program_id(0)

    def fetch(k):
        return pltpu.make_async_copy(windows[k], held.at[k], sems.at[k])

    @pl.when(at == 0)
    def _():
        for k in range(count):
            fetch(k).start()

    for k in range(count):
        pl.when(at == k)(lambda k=k: fetch(k).wait())

    even = ((base + at) & 1) == 0
    window = held.at[at]
    span = held.shape[1] - DOCS
    slots = ROUNDS * R
    rows = COLS * slots

    def load(refs_of, lanes):
        last = jnp.where(even, refs_of[3][:, lanes], refs_of[4][:, lanes])
        return [ref[:, lanes].astype(jnp.float32) for ref in refs_of[:3]] + [
            last.astype(jnp.float32)
        ]

    marks = window[span:, : 2 * HD].astype(jnp.float32)
    starts = marks[:, :HD] * 16.0 + marks[:, HD:]
    place = jnp.concatenate(load(place_refs, slice(0, HD)), axis=0) + float(BEHIND * HD)
    first = jnp.zeros_like(place)
    for doc in range(DOCS):
        start = jnp.broadcast_to(starts[doc : doc + 1, :], place.shape)
        first = jnp.maximum(first, jnp.where(start <= place, start, 0.0))
    lane = lax.broadcasted_iota(jnp.int32, place.shape, 1).astype(jnp.float32)
    bias = []
    for tile in range(span // HD):
        key_pos = lane + float(tile * HD)
        allowed = (key_pos >= first) & (key_pos <= place)
        bias.append(jnp.where(allowed, 0.0, -1e30))
    bias = jnp.concatenate(bias, axis=1)
    per_part = GROUPS // PARTS
    for head in range(KVH):
        keys = window[:span, 2 * head * HD : (2 * head + 1) * HD]
        values = window[:span, (2 * head + 1) * HD : (2 * head + 2) * HD]
        for part in range(PARTS):
            first_head = head * GROUPS + part * per_part
            heads = range(first_head, first_head + per_part)
            query = jnp.concatenate(
                [piece for h in heads for piece in load(query_refs, slice(h * HD, (h + 1) * HD))],
                axis=0,
            ).astype(jnp.bfloat16)
            scores = lax.dot_general(
                query, keys, (((1,), (1,)), ((), ())), preferred_element_type=jnp.float32
            )
            weights, inverse = [], []
            for n in range(per_part):
                scaled = scores[n * rows : (n + 1) * rows] * SCALE + bias
                weight = jnp.exp2(scaled - jnp.max(scaled, axis=1, keepdims=True))
                inverse.append(1.0 / jnp.sum(weight, axis=1, keepdims=True))
                weights.append(weight.astype(jnp.bfloat16))
            weighted = lax.dot_general(
                jnp.concatenate(weights, axis=0),
                values,
                (((1,), (0,)), ((), ())),
                preferred_element_type=jnp.float32,
            )
            for n, h in enumerate(heads):
                result = weighted[n * rows : (n + 1) * rows] * inverse[n]
                for c in range(COLS):
                    piece = result[c * slots : (c + 1) * slots].astype(jnp.bfloat16)
                    ref = far if c == COLS - 1 else out_refs[c]
                    ref[:, h * HD : (h + 1) * HD] = piece
    for ref, group in zip(out_refs[3:], groups_out[3:]):

        @pl.when(even if group == 3 else jnp.logical_not(even))
        def _(ref=ref):
            ref[...] = far[...]


def far_orders(group, orders):
    return [order for order in orders if order % 2 == group - 3]


def attend(arrived, windows, orders, batch, buffers):
    slots = ROUNDS * R
    width = QH * HD
    base, count = orders[0], len(orders)
    spots = [lambda i: base + i] * 3 + [lambda i: (base + i) >> 1] * 2
    groups_out = [0, 1, 2] + [group for group in (3, 4) if far_orders(group, orders)]
    out_specs, out_shape = [], []
    for group in groups_out:
        if group < 3:
            total = len(batch)
            spot = lambda i: base - batch[0] + i
        else:
            mine = far_orders(group, batch)
            total, lowest = len(mine), mine[0] // 2
            shift = 1 if group == 3 else 0
            spot = lambda i, t=total, l=lowest, s=shift: jnp.clip(((base + i + s) >> 1) - l, 0, t - 1)
        out_specs.append(pl.BlockSpec((slots, width), lambda i, spot=spot: (spot(i), 0)))
        out_shape.append(jax.ShapeDtypeStruct((total * slots, width), jnp.bfloat16))
    kept = [group for group in groups_out if group in buffers]
    anywhere = pl.BlockSpec(memory_space=pl.ANY)
    outs = pl.pallas_call(
        lambda *refs: attend_kernel(base, count, groups_out, len(kept), *refs),
        grid=(count,),
        in_specs=[pl.BlockSpec((slots, width), lambda i, spot=spot: (spot(i), 0)) for spot in spots]
        + [
            pl.BlockSpec((slots, HD), lambda i, spot=spot: (spot(i), width // HD))
            for spot in spots
        ]
        + [anywhere] * (count + len(kept)),
        out_specs=out_specs,
        out_shape=out_shape,
        scratch_shapes=[
            pltpu.VMEM((count,) + windows[0].shape, jnp.bfloat16),
            pltpu.VMEM((slots, width), jnp.bfloat16),
            pltpu.SemaphoreType.DMA((count,)),
        ],
        input_output_aliases={10 + count + n: groups_out.index(g) for n, g in enumerate(kept)},
        compiler_params=pltpu.CompilerParams(dimension_semantics=("arbitrary",)),
    )(*arrived, *arrived, *windows, *[buffers[group] for group in kept])
    return {**buffers, **dict(zip(groups_out, outs))}


def collect_kernel(select_ref, *refs):
    backs, out_ref = refs[:-1], refs[-1]
    joined = jnp.concatenate([ref[...].astype(jnp.float32) for ref in backs], axis=0)
    out_ref[...] = jnp.dot(
        select_ref[...], joined.astype(jnp.bfloat16), preferred_element_type=jnp.float32
    ).astype(jnp.bfloat16)


def collect(select, backs):
    rows, width = select.shape[0], backs[0].shape[1]
    chunk = width // 4
    return pl.pallas_call(
        collect_kernel,
        grid=(4,),
        in_specs=[pl.BlockSpec(select.shape, lambda i: (0, 0))]
        + [pl.BlockSpec((back.shape[0], chunk), lambda i: (0, i)) for back in backs],
        out_specs=pl.BlockSpec((rows, chunk), lambda i: (0, i)),
        out_shape=jax.ShapeDtypeStruct((rows, width), jnp.bfloat16),
        compiler_params=pltpu.CompilerParams(dimension_semantics=("arbitrary",)),
        name="collect",
    )(select, *backs)


def along_z(array, by):
    planes = lax.axis_size("z")
    return lax.ppermute(array, "z", [(i, (i + by) % planes) for i in range(planes)])


def along_y(array, by):
    ring = 2 * COLS
    spot = [(i % COLS) * 2 + i // COLS for i in range(ring)]
    pairs = [(spot[i], spot[(i + by) % ring]) for i in range(ring)]
    return lax.ppermute(array, ("col", "yh"), pairs)


def along_x(array, by):
    peers = lax.axis_size("x")
    return lax.ppermute(array, "x", [(i, i + by) for i in range(peers - by)])


def window_of(key_rows, value_rows, lengths):
    x, upper = lax.axis_index("x"), lax.axis_index("yh")
    key, value = key_rows[0], value_rows[0]
    block = key.shape[0]
    joined = jnp.concatenate([key[:, :HD], value[:, :HD], key[:, HD:], value[:, HD:]], axis=1)
    other = lax.ppermute(joined, "yh", [(0, 1), (1, 0)])
    lower_block = jnp.where(upper == 0, joined, other)
    upper_block = jnp.where(upper == 0, other, joined)
    pair = jnp.concatenate([lower_block, upper_block], axis=0)
    pair_behind = along_x(pair, 1)
    last_behind = along_x(upper_block, 2)
    origin = (2 * x - BEHIND) * block
    lowest = jnp.maximum(0, -origin)
    ends = jnp.cumsum(lengths[0])[:-1] - origin
    starts = jnp.concatenate([lowest[None], jnp.clip(ends, lowest, (BEHIND + 2) * block)])
    high = jnp.broadcast_to((starts // 16)[:, None], (DOCS, HD))
    low = jnp.broadcast_to((starts % 16)[:, None], (DOCS, HD))
    marks = jnp.concatenate([high, low, high, low], axis=1).astype(jnp.bfloat16)
    return jnp.concatenate([last_behind, pair_behind, pair, marks], axis=0)


def pick(select, array):
    return jnp.dot(select, array, preferred_element_type=jnp.float32).astype(jnp.bfloat16)


def on_device(queries, destination, offsets, key_rows, value_rows, lengths):
    planes = lax.axis_size("z")
    column, plane = lax.axis_index("col"), lax.axis_index("z")
    upper = lax.axis_index("yh")
    block = key_rows.shape[1]
    rows = destination.shape[2] * R
    slots = ROUNDS * R
    reach = planes // 2
    window = window_of(key_rows, value_rows, lengths)

    target = jnp.repeat(destination[0, 0], R)
    row = jnp.arange(rows, dtype=jnp.int32)
    ahead = (target // COLS - plane) % planes
    order = jnp.where(ahead <= reach, jnp.maximum(2 * ahead - 1, 0), 2 * (planes - ahead))
    within = (row // (rows // ROUNDS)) * R + row % R
    across = (target % COLS - column) % COLS
    place = upper * block + jnp.repeat(offsets[0, 0], R) + row % R
    place = jnp.broadcast_to(place[:, None], (rows, HD)).astype(jnp.bfloat16)
    payload = jnp.concatenate([queries[0, 0], place], axis=1)
    groups = [
        (across == 0, order, 0),
        (across == 1, order, 1),
        (across == 3, order, -1),
        ((across == 2) & (order % 2 == 0), order // 2, 2),
        ((across == 2) & (order % 2 == 1), order // 2, -2),
    ]
    selects, arrived = [], []
    for number, (chosen, at, by) in enumerate(groups):
        count = (planes if number < 3 else reach) * slots
        slot = jnp.arange(count, dtype=jnp.int32)[:, None]
        select = (((at * slots + within)[None, :] == slot) & chosen[None, :]).astype(jnp.bfloat16)
        selects.append(select)
        sending = pick(select, payload)
        arrived.append(along_y(sending, by) if by else sending)

    windows = [window]
    ahead_window, behind_window = window, window
    width = window.shape[1] // 2
    backs, chosen = [], []

    def serve(orders, batch, buffers):
        return attend(arrived, [windows[order] for order in orders], orders, batch, buffers)

    def give_back(buffers, batch):
        for number, (_, _, by) in enumerate(groups):
            orders = batch if number < 3 else far_orders(number, batch)
            lowest = orders[0] if number < 3 else orders[0] // 2
            backs.append(along_y(buffers[number], -by) if by else buffers[number])
            chosen.append(selects[number][lowest * slots : (lowest + len(orders)) * slots])

    early = list(range(planes - 3))
    late = list(range(planes - 3, planes))
    for _ in range(1, reach):
        ahead_window = along_z(ahead_window, -1)
        behind_window = along_z(behind_window, 1)
        windows += [ahead_window, behind_window]
    last_left = along_z(ahead_window[:, :width], -1)
    last_right = along_z(behind_window[:, width:], 1)
    windows.append(jnp.concatenate([last_left, last_right], axis=1))

    buffers = serve(early[:-2], early, {})
    buffers = serve(early[-2:], early, buffers)
    give_back(buffers, early)
    buffers = serve(late[:2], late, {})
    buffers = serve(late[2:], late, buffers)
    give_back(buffers, late)
    return collect(jnp.concatenate(chosen, axis=0).T, backs)[None, None]


def solution(mesh):
    shape = dict(mesh.shape)
    fine = Mesh(
        mesh.devices.reshape(shape["srv"] // COLS, COLS, shape["blk"] // 2, 2, shape["rep"]),
        ("z", "col", "x", "yh", "rep"),
    )
    srv, blk = ("z", "col"), ("x", "yh")
    placed = (
        P(srv, blk, "rep", None),
        P(srv, blk, "rep"),
        P(srv, blk, "rep"),
        P(srv, blk, "rep"),
        P(srv, blk, "rep"),
        P(srv, "rep"),
    )

    return jax.shard_map(
        on_device,
        mesh=fine,
        in_specs=placed,
        out_specs=P(srv, blk, "rep", None),
        check_vma=False,
    )
```

```python
import math

import jax
import jax.numpy as jnp
from jax import lax
from jax.experimental import pallas as pl
from jax.experimental.pallas import tpu as pltpu
from jax.sharding import Mesh
from jax.sharding import PartitionSpec as P

QH = 32
KVH = 2
HD = 128
R = 4
ROUNDS = 2
COLS = 4
GROUPS = QH // KVH
DOCS = 8
BEHIND = 3
PARTS = 1
SCALE = math.log2(math.e) / math.sqrt(HD)


def attend_kernel(base, count, split, sources, groups_out, aliased, *refs):
    query_refs, place_refs = refs[:sources], refs[sources : 2 * sources]
    sizes = [1] * (count - split) + [2] * split
    at_ref = 2 * sources
    windows = []
    for size in sizes:
        windows.append(refs[at_ref : at_ref + size])
        at_ref += size
    at_ref += aliased
    out_refs = refs[at_ref : at_ref + len(groups_out)]
    held, far, sems = refs[at_ref + len(groups_out) :]
    at = pl.program_id(0)
    mixed = sources == 5

    def fetches(k):
        pieces = windows[k]
        width = held.shape[2] // len(pieces)
        return [
            pltpu.make_async_copy(
                piece, held.at[k, :, n * width : (n + 1) * width], sems.at[k, n]
            )
            for n, piece in enumerate(pieces)
        ]

    @pl.when(at == 0)
    def _():
        for k in range(count):
            for copy in fetches(k):
                copy.start()

    for k in range(count):

        @pl.when(at == k)
        def _(k=k):
            for copy in fetches(k):
                copy.wait()

    even = ((base + at) & 1) == 0
    window = held.at[at]
    span = held.shape[1] - DOCS
    slots = ROUNDS * R
    rows = COLS * slots

    def load(refs_of, lanes):
        if mixed:
            last = jnp.where(even, refs_of[3][:, lanes], refs_of[4][:, lanes])
        else:
            last = refs_of[3][:, lanes]
        return [ref[:, lanes].astype(jnp.float32) for ref in refs_of[:3]] + [
            last.astype(jnp.float32)
        ]

    marks = window[span:, : 2 * HD].astype(jnp.float32)
    starts = marks[:, :HD] * 16.0 + marks[:, HD:]
    place = jnp.concatenate(load(place_refs, slice(0, HD)), axis=0) + float(BEHIND * HD)
    first = jnp.zeros_like(place)
    for doc in range(DOCS):
        start = jnp.broadcast_to(starts[doc : doc + 1, :], place.shape)
        first = jnp.maximum(first, jnp.where(start <= place, start, 0.0))
    lane = lax.broadcasted_iota(jnp.int32, place.shape, 1).astype(jnp.float32)
    bias = []
    for tile in range(span // HD):
        key_pos = lane + float(tile * HD)
        allowed = (key_pos >= first) & (key_pos <= place)
        bias.append(jnp.where(allowed, 0.0, -1e30))
    bias = jnp.concatenate(bias, axis=1)
    per_part = GROUPS // PARTS
    for head in range(KVH):
        keys = window[:span, 2 * head * HD : (2 * head + 1) * HD]
        values = window[:span, (2 * head + 1) * HD : (2 * head + 2) * HD]
        for part in range(PARTS):
            first_head = head * GROUPS + part * per_part
            heads = range(first_head, first_head + per_part)
            query = jnp.concatenate(
                [piece for h in heads for piece in load(query_refs, slice(h * HD, (h + 1) * HD))],
                axis=0,
            ).astype(jnp.bfloat16)
            scores = lax.dot_general(
                query, keys, (((1,), (1,)), ((), ())), preferred_element_type=jnp.float32
            )
            weights, inverse = [], []
            for n in range(per_part):
                scaled = scores[n * rows : (n + 1) * rows] * SCALE + bias
                weight = jnp.exp2(scaled - jnp.max(scaled, axis=1, keepdims=True))
                inverse.append(1.0 / jnp.sum(weight, axis=1, keepdims=True))
                weights.append(weight.astype(jnp.bfloat16))
            weighted = lax.dot_general(
                jnp.concatenate(weights, axis=0),
                values,
                (((1,), (0,)), ((), ())),
                preferred_element_type=jnp.float32,
            )
            for n, h in enumerate(heads):
                result = weighted[n * rows : (n + 1) * rows] * inverse[n]
                for c in range(COLS):
                    piece = result[c * slots : (c + 1) * slots].astype(jnp.bfloat16)
                    ref = far if mixed and c == COLS - 1 else out_refs[c]
                    ref[:, h * HD : (h + 1) * HD] = piece
    if mixed:

        @pl.when(even)
        def _():
            out_refs[3][...] = far[...]

        @pl.when(jnp.logical_not(even))
        def _():
            out_refs[4][...] = far[...]


def attend(arrived, windows, orders, batch, buffers):
    slots = ROUNDS * R
    width = QH * HD
    base, count, start = orders[0], len(orders), batch[0]
    by_order = lambda i: base + i
    if start == 0:
        evens, odds = (len(batch) + 1) // 2, len(batch) // 2
        spots = [by_order] * 3 + [lambda i: (base + i) >> 1] * 2
        groups_out = [0, 1, 2, 3, 4]
        totals = [len(batch)] * 3 + [evens, odds]
        places = [by_order] * 3 + [
            lambda i: jnp.minimum((base + i + 1) >> 1, evens - 1),
            lambda i: jnp.minimum((base + i) >> 1, odds - 1),
        ]
        spots[3] = lambda i: jnp.minimum((base + i) >> 1, evens - 1)
    else:
        spots = [by_order] * 3 + [lambda i: base - start + start // 2 + i]
        groups_out = [0, 1, 2, 4]
        totals = [len(batch)] * 4
        places = [lambda i: base - start + i] * 4
    sources = [arrived[group] for group in groups_out]
    out_specs = [
        pl.BlockSpec((slots, width), lambda i, place=place: (place(i), 0)) for place in places
    ]
    out_shape = [jax.ShapeDtypeStruct((total * slots, width), jnp.bfloat16) for total in totals]
    pieces = [piece for window in windows for piece in window]
    split = sum(len(window) == 2 for window in windows)
    kept = [buffers[group] for group in groups_out if group in buffers]
    shape = (pieces[0].shape[0], sum(piece.shape[1] for piece in windows[0]))
    anywhere = pl.BlockSpec(memory_space=pl.ANY)
    known = 2 * len(sources) + len(pieces)
    outs = pl.pallas_call(
        lambda *refs: attend_kernel(
            base, count, split, len(sources), groups_out, len(kept), *refs
        ),
        grid=(count,),
        in_specs=[pl.BlockSpec((slots, width), lambda i, spot=spot: (spot(i), 0)) for spot in spots]
        + [
            pl.BlockSpec((slots, HD), lambda i, spot=spot: (spot(i), width // HD))
            for spot in spots
        ]
        + [anywhere] * (len(pieces) + len(kept)),
        out_specs=out_specs,
        out_shape=out_shape,
        scratch_shapes=[
            pltpu.VMEM((count,) + shape, jnp.bfloat16),
            pltpu.VMEM((slots, width), jnp.bfloat16),
            pltpu.SemaphoreType.DMA((count, 2)),
        ],
        input_output_aliases={known + n: n for n in range(len(kept))},
        compiler_params=pltpu.CompilerParams(dimension_semantics=("arbitrary",)),
    )(*sources, *sources, *pieces, *kept)
    return dict(zip(groups_out, outs))


def collect_kernel(partial, select_ref, *refs):
    backs, out_ref = refs[partial:-1], refs[-1]
    joined = jnp.concatenate([ref[...].astype(jnp.float32) for ref in backs], axis=0)
    total = jnp.dot(
        select_ref[...], joined.astype(jnp.bfloat16), preferred_element_type=jnp.float32
    )
    if partial:
        total = total + refs[0][...].astype(jnp.float32)
    out_ref[...] = total.astype(jnp.bfloat16)


def collect(select, backs, partial):
    rows, width = select.shape[0], backs[0].shape[1]
    chunk = width // 4
    whole = pl.BlockSpec((rows, chunk), lambda i: (0, i))
    return pl.pallas_call(
        lambda *refs: collect_kernel(len(partial), *refs),
        grid=(4,),
        in_specs=[pl.BlockSpec(select.shape, lambda i: (0, 0))]
        + [whole] * len(partial)
        + [pl.BlockSpec((back.shape[0], chunk), lambda i: (0, i)) for back in backs],
        out_specs=whole,
        out_shape=jax.ShapeDtypeStruct((rows, width), jnp.bfloat16),
        compiler_params=pltpu.CompilerParams(dimension_semantics=("arbitrary",)),
    )(select, *partial, *backs)


def along_z(array, by):
    planes = lax.axis_size("z")
    return lax.ppermute(array, "z", [(i, (i + by) % planes) for i in range(planes)])


def along_y(array, by):
    ring = 2 * COLS
    spot = [(i % COLS) * 2 + i // COLS for i in range(ring)]
    pairs = [(spot[i], spot[(i + by) % ring]) for i in range(ring)]
    return lax.ppermute(array, ("col", "yh"), pairs)


def along_x(array, by):
    peers = lax.axis_size("x")
    return lax.ppermute(array, "x", [(i, i + by) for i in range(peers - by)])


def window_of(key_rows, value_rows, lengths):
    x, upper = lax.axis_index("x"), lax.axis_index("yh")
    key, value = key_rows[0], value_rows[0]
    block = key.shape[0]
    joined = jnp.concatenate([key[:, :HD], value[:, :HD], key[:, HD:], value[:, HD:]], axis=1)
    other = lax.ppermute(joined, "yh", [(0, 1), (1, 0)])
    lower_block = jnp.where(upper == 0, joined, other)
    upper_block = jnp.where(upper == 0, other, joined)
    pair = jnp.concatenate([lower_block, upper_block], axis=0)
    pair_behind = along_x(pair, 1)
    last_behind = along_x(upper_block, 2)
    origin = (2 * x - BEHIND) * block
    lowest = jnp.maximum(0, -origin)
    ends = jnp.cumsum(lengths[0])[:-1] - origin
    starts = jnp.concatenate([lowest[None], jnp.clip(ends, lowest, (BEHIND + 2) * block)])
    high = jnp.broadcast_to((starts // 16)[:, None], (DOCS, HD))
    low = jnp.broadcast_to((starts % 16)[:, None], (DOCS, HD))
    marks = jnp.concatenate([high, low, high, low], axis=1).astype(jnp.bfloat16)
    return jnp.concatenate([last_behind, pair_behind, pair, marks], axis=0)


def pick(select, array):
    return jnp.dot(select, array, preferred_element_type=jnp.float32).astype(jnp.bfloat16)


def on_device(queries, destination, offsets, key_rows, value_rows, lengths):
    planes = lax.axis_size("z")
    column, plane = lax.axis_index("col"), lax.axis_index("z")
    upper = lax.axis_index("yh")
    block = key_rows.shape[1]
    rows = destination.shape[2] * R
    slots = ROUNDS * R
    reach = planes // 2
    window = window_of(key_rows, value_rows, lengths)

    target = jnp.repeat(destination[0, 0], R)
    row = jnp.arange(rows, dtype=jnp.int32)
    ahead = (target // COLS - plane) % planes
    order = jnp.where(ahead <= reach, jnp.maximum(2 * ahead - 1, 0), 2 * (planes - ahead))
    within = (row // (rows // ROUNDS)) * R + row % R
    across = (target % COLS - column) % COLS
    place = upper * block + jnp.repeat(offsets[0, 0], R) + row % R
    place = jnp.broadcast_to(place[:, None], (rows, HD)).astype(jnp.bfloat16)
    payload = jnp.concatenate([queries[0, 0], place], axis=1)
    late_start = planes - 3
    late = order >= late_start
    even = order % 2 == 0
    minus = jnp.where(late, order - late_start + late_start // 2, order // 2)
    evens = (late_start + 1) // 2
    groups = [
        (across == 0, order, planes, 0),
        (across == 1, order, planes, 1),
        (across == 3, order, planes, -1),
        ((across == 2) & even & ~late, order // 2, evens, 2),
        ((across == 2) & (late | ~even), minus, planes - evens, -2),
    ]
    arrived = []
    spot_early, spot_late = jnp.full((rows,), -1, jnp.int32), jnp.full((rows,), -1, jnp.int32)
    base_early, base_late = 0, 0
    for number, (chosen, at, count, by) in enumerate(groups):
        slot = jnp.arange(count * slots, dtype=jnp.int32)[:, None]
        select = (((at * slots + within)[None, :] == slot) & chosen[None, :]).astype(jnp.bfloat16)
        sending = pick(select, payload)
        arrived.append(along_y(sending, by) if by else sending)
        spot_early = jnp.where(chosen & ~late, base_early + at * slots + within, spot_early)
        base_early += slots * (late_start if number < 3 else (evens if number == 3 else late_start // 2))
        if number != 3:
            at_late = base_late + (order - late_start) * slots + within
            spot_late = jnp.where(chosen & late, at_late, spot_late)
            base_late += slots * 3
    select_early = (spot_early[:, None] == jnp.arange(base_early)[None, :]).astype(jnp.bfloat16)
    select_late = (spot_late[:, None] == jnp.arange(base_late)[None, :]).astype(jnp.bfloat16)

    windows = [(window,)]
    ahead_window, behind_window = window, window
    width = window.shape[1] // 2
    for _ in range(1, reach):
        ahead_window = along_z(ahead_window, -1)
        behind_window = along_z(behind_window, 1)
        windows += [(ahead_window,), (behind_window,)]
    last_left = along_z(ahead_window[:, :width], -1)
    last_right = along_z(behind_window[:, width:], 1)
    windows.append((last_left, last_right))

    def serve(orders, batch, buffers):
        return attend(arrived, [windows[order] for order in orders], orders, batch, buffers)

    def give_back(buffers):
        backs = []
        for number, (_, _, _, by) in enumerate(groups):
            if number in buffers:
                backs.append(along_y(buffers[number], -by) if by else buffers[number])
        return backs

    early_orders, late_orders = list(range(late_start)), list(range(late_start, planes))
    buffers = serve(early_orders[:3], early_orders, {})
    for step in range(2, reach - 1):
        buffers = serve([2 * step - 1, 2 * step], early_orders, buffers)
    early_backs = give_back(buffers)
    buffers = serve(late_orders[:2], late_orders, {})
    buffers = serve(late_orders[2:], late_orders, buffers)
    late_backs = give_back(buffers)
    partial = collect(select_early, early_backs, [])
    return collect(select_late, late_backs, [partial])[None, None]


def solution(mesh):
    shape = dict(mesh.shape)
    fine = Mesh(
        mesh.devices.reshape(shape["srv"] // COLS, COLS, shape["blk"] // 2, 2, shape["rep"]),
        ("z", "col", "x", "yh", "rep"),
    )
    srv, blk = ("z", "col"), ("x", "yh")
    placed = (
        P(srv, blk, "rep", None),
        P(srv, blk, "rep"),
        P(srv, blk, "rep"),
        P(srv, blk, "rep"),
        P(srv, blk, "rep"),
        P(srv, "rep"),
    )

    return jax.shard_map(
        on_device,
        mesh=fine,
        in_specs=placed,
        out_specs=P(srv, blk, "rep", None),
        check_vma=False,
    )
```

```python
import math

import jax
import jax.numpy as jnp
from jax import lax
from jax.experimental import pallas as pl
from jax.experimental.pallas import tpu as pltpu
from jax.sharding import Mesh
from jax.sharding import PartitionSpec as P

QH = 32
KVH = 2
HD = 128
R = 4
ROUNDS = 2
COLS = 4
GROUPS = QH // KVH
DOCS = 8
BEHIND = 3
PARTS = 1
SCALE = math.log2(math.e) / math.sqrt(HD)


def fetched(at, windows, held, sems):
    def fetches(k):
        pieces = windows[k]
        width = held.shape[2] // len(pieces)
        return [
            pltpu.make_async_copy(
                piece, held.at[k, :, n * width : (n + 1) * width], sems.at[k, n]
            )
            for n, piece in enumerate(pieces)
        ]

    @pl.when(at == 0)
    def _():
        for k in range(len(windows)):
            for copy in fetches(k):
                copy.start()

    for k in range(len(windows)):

        @pl.when(at == k)
        def _(k=k):
            for copy in fetches(k):
                copy.wait()

    return held.at[at]


def attend_kernel(base, count, split, sources, groups_out, aliased, *refs):
    query_refs, place_refs = refs[:sources], refs[sources : 2 * sources]
    sizes = [1] * (count - split) + [2] * split
    at_ref = 2 * sources
    windows = []
    for size in sizes:
        windows.append(refs[at_ref : at_ref + size])
        at_ref += size
    at_ref += aliased
    out_refs = refs[at_ref : at_ref + len(groups_out)]
    far = refs[at_ref + len(groups_out)]
    at = pl.program_id(0)
    mixed = sources == 5
    even = ((base + at) & 1) == 0
    if count > 2:
        held, sems = refs[at_ref + len(groups_out) + 1 :]
        window = fetched(at, windows, held, sems)
        full = window.shape[0]

        def columns(number, where):
            return window[where, number * HD : (number + 1) * HD]

    else:
        full = windows[0][0].shape[0]

        def columns(number, where):
            pieces = []
            for window in windows:
                width = window[0].shape[1]
                lane = number * HD % width
                pieces.append(window[number * HD // width][where, lane : lane + HD])
            return pieces[0] if count == 1 else jnp.where(at == 0, pieces[0], pieces[1])

    span = full - DOCS
    slots = ROUNDS * R
    rows = COLS * slots

    def load(refs_of, lanes):
        if mixed:
            last = jnp.where(even, refs_of[3][:, lanes], refs_of[4][:, lanes])
        else:
            last = refs_of[3][:, lanes]
        return [ref[:, lanes].astype(jnp.float32) for ref in refs_of[:3]] + [
            last.astype(jnp.float32)
        ]

    marks = slice(span, full)
    starts = columns(0, marks).astype(jnp.float32) * 16.0 + columns(1, marks).astype(jnp.float32)
    place = jnp.concatenate(load(place_refs, slice(0, HD)), axis=0) + float(BEHIND * HD)
    first = jnp.zeros_like(place)
    for doc in range(DOCS):
        start = jnp.broadcast_to(starts[doc : doc + 1, :], place.shape)
        first = jnp.maximum(first, jnp.where(start <= place, start, 0.0))
    lane = lax.broadcasted_iota(jnp.int32, place.shape, 1).astype(jnp.float32)
    bias = []
    for tile in range(span // HD):
        key_pos = lane + float(tile * HD)
        allowed = (key_pos >= first) & (key_pos <= place)
        bias.append(jnp.where(allowed, 0.0, -1e30))
    bias = jnp.concatenate(bias, axis=1)
    per_part = GROUPS // PARTS
    for head in range(KVH):
        keys = columns(2 * head, slice(0, span))
        values = columns(2 * head + 1, slice(0, span))
        for part in range(PARTS):
            first_head = head * GROUPS + part * per_part
            heads = range(first_head, first_head + per_part)
            query = jnp.concatenate(
                [piece for h in heads for piece in load(query_refs, slice(h * HD, (h + 1) * HD))],
                axis=0,
            ).astype(jnp.bfloat16)
            scores = lax.dot_general(
                query, keys, (((1,), (1,)), ((), ())), preferred_element_type=jnp.float32
            )
            weights, inverse = [], []
            for n in range(per_part):
                scaled = scores[n * rows : (n + 1) * rows] * SCALE + bias
                weight = jnp.exp2(scaled - jnp.max(scaled, axis=1, keepdims=True))
                inverse.append(1.0 / jnp.sum(weight, axis=1, keepdims=True))
                weights.append(weight.astype(jnp.bfloat16))
            weighted = lax.dot_general(
                jnp.concatenate(weights, axis=0),
                values,
                (((1,), (0,)), ((), ())),
                preferred_element_type=jnp.float32,
            )
            for n, h in enumerate(heads):
                result = weighted[n * rows : (n + 1) * rows] * inverse[n]
                for c in range(COLS):
                    piece = result[c * slots : (c + 1) * slots].astype(jnp.bfloat16)
                    ref = far if mixed and c == COLS - 1 else out_refs[c]
                    ref[:, h * HD : (h + 1) * HD] = piece
    if mixed:

        @pl.when(even)
        def _():
            out_refs[3][...] = far[...]

        @pl.when(jnp.logical_not(even))
        def _():
            out_refs[4][...] = far[...]


def attend(arrived, windows, orders, batch, buffers):
    slots = ROUNDS * R
    width = QH * HD
    base, count, start = orders[0], len(orders), batch[0]
    by_order = lambda i: base + i
    if start == 0:
        evens, odds = (len(batch) + 1) // 2, len(batch) // 2
        spots = [by_order] * 3 + [lambda i: (base + i) >> 1] * 2
        groups_out = [0, 1, 2, 3, 4]
        totals = [len(batch)] * 3 + [evens, odds]
        places = [by_order] * 3 + [
            lambda i: jnp.minimum((base + i + 1) >> 1, evens - 1),
            lambda i: jnp.minimum((base + i) >> 1, odds - 1),
        ]
        spots[3] = lambda i: jnp.minimum((base + i) >> 1, evens - 1)
    else:
        spots = [by_order] * 3 + [lambda i: base - start + start // 2 + i]
        groups_out = [0, 1, 2, 4]
        totals = [len(batch)] * 4
        places = [lambda i: base - start + i] * 4
    sources = [arrived[group] for group in groups_out]
    out_specs = [
        pl.BlockSpec((slots, width), lambda i, place=place: (place(i), 0)) for place in places
    ]
    out_shape = [jax.ShapeDtypeStruct((total * slots, width), jnp.bfloat16) for total in totals]
    pieces = [piece for window in windows for piece in window]
    split = sum(len(window) == 2 for window in windows)
    kept = [buffers[group] for group in groups_out if group in buffers]
    shape = (pieces[0].shape[0], sum(piece.shape[1] for piece in windows[0]))
    anywhere = pl.BlockSpec(memory_space=pl.ANY)
    known = 2 * len(sources) + len(pieces)
    outs = pl.pallas_call(
        lambda *refs: attend_kernel(
            base, count, split, len(sources), groups_out, len(kept), *refs
        ),
        grid=(count,),
        in_specs=[pl.BlockSpec((slots, width), lambda i, spot=spot: (spot(i), 0)) for spot in spots]
        + [
            pl.BlockSpec((slots, HD), lambda i, spot=spot: (spot(i), width // HD))
            for spot in spots
        ]
        + [
            anywhere if count > 2 else pl.BlockSpec(piece.shape, lambda i: (0, 0))
            for piece in pieces
        ]
        + [anywhere] * len(kept),
        out_specs=out_specs,
        out_shape=out_shape,
        scratch_shapes=[pltpu.VMEM((slots, width), jnp.bfloat16)]
        + (
            [
                pltpu.VMEM((count,) + shape, jnp.bfloat16),
                pltpu.SemaphoreType.DMA((count, 2)),
            ]
            if count > 2
            else []
        ),
        input_output_aliases={known + n: n for n in range(len(kept))},
        compiler_params=pltpu.CompilerParams(dimension_semantics=("arbitrary",)),
    )(*sources, *sources, *pieces, *kept)
    return dict(zip(groups_out, outs))


def collect_kernel(partial, select_ref, *refs):
    backs, out_ref = refs[partial:-1], refs[-1]
    joined = jnp.concatenate([ref[...].astype(jnp.float32) for ref in backs], axis=0)
    total = jnp.dot(
        select_ref[...], joined.astype(jnp.bfloat16), preferred_element_type=jnp.float32
    )
    if partial:
        total = total + refs[0][...].astype(jnp.float32)
    out_ref[...] = total.astype(jnp.bfloat16)


def collect(select, backs, partial):
    rows, width = select.shape[0], backs[0].shape[1]
    chunk = width // 2
    whole = pl.BlockSpec((rows, chunk), lambda i: (0, i))
    return pl.pallas_call(
        lambda *refs: collect_kernel(len(partial), *refs),
        grid=(2,),
        in_specs=[pl.BlockSpec(select.shape, lambda i: (0, 0))]
        + [whole] * len(partial)
        + [pl.BlockSpec((back.shape[0], chunk), lambda i: (0, i)) for back in backs],
        out_specs=whole,
        out_shape=jax.ShapeDtypeStruct((rows, width), jnp.bfloat16),
        compiler_params=pltpu.CompilerParams(dimension_semantics=("arbitrary",)),
    )(select, *partial, *backs)


def along_z(array, by):
    planes = lax.axis_size("z")
    return lax.ppermute(array, "z", [(i, (i + by) % planes) for i in range(planes)])


def along_y(array, by):
    ring = 2 * COLS
    spot = [(i % COLS) * 2 + i // COLS for i in range(ring)]
    pairs = [(spot[i], spot[(i + by) % ring]) for i in range(ring)]
    return lax.ppermute(array, ("col", "yh"), pairs)


def along_x(array, by):
    peers = lax.axis_size("x")
    return lax.ppermute(array, "x", [(i, i + by) for i in range(peers - by)])


def window_of(key_rows, value_rows, lengths):
    x, upper = lax.axis_index("x"), lax.axis_index("yh")
    key, value = key_rows[0], value_rows[0]
    block = key.shape[0]
    joined = jnp.concatenate([key[:, :HD], value[:, :HD], key[:, HD:], value[:, HD:]], axis=1)
    other = lax.ppermute(joined, "yh", [(0, 1), (1, 0)])
    lower_block = jnp.where(upper == 0, joined, other)
    upper_block = jnp.where(upper == 0, other, joined)
    pair = jnp.concatenate([lower_block, upper_block], axis=0)
    pair_behind = along_x(pair, 1)
    last_behind = along_x(upper_block, 2)
    origin = (2 * x - BEHIND) * block
    lowest = jnp.maximum(0, -origin)
    ends = jnp.cumsum(lengths[0])[:-1] - origin
    starts = jnp.concatenate([lowest[None], jnp.clip(ends, lowest, (BEHIND + 2) * block)])
    high = jnp.broadcast_to((starts // 16)[:, None], (DOCS, HD))
    low = jnp.broadcast_to((starts % 16)[:, None], (DOCS, HD))
    marks = jnp.concatenate([high, low, high, low], axis=1).astype(jnp.bfloat16)
    return jnp.concatenate([last_behind, pair_behind, pair, marks], axis=0)


def pick(select, array):
    return jnp.dot(select, array, preferred_element_type=jnp.float32).astype(jnp.bfloat16)


def on_device(queries, destination, offsets, key_rows, value_rows, lengths):
    planes = lax.axis_size("z")
    column, plane = lax.axis_index("col"), lax.axis_index("z")
    upper = lax.axis_index("yh")
    block = key_rows.shape[1]
    rows = destination.shape[2] * R
    slots = ROUNDS * R
    reach = planes // 2
    window = window_of(key_rows, value_rows, lengths)

    target = jnp.repeat(destination[0, 0], R)
    row = jnp.arange(rows, dtype=jnp.int32)
    ahead = (target // COLS - plane) % planes
    order = jnp.where(ahead <= reach, jnp.maximum(2 * ahead - 1, 0), 2 * (planes - ahead))
    within = (row // (rows // ROUNDS)) * R + row % R
    across = (target % COLS - column) % COLS
    place = upper * block + jnp.repeat(offsets[0, 0], R) + row % R
    place = jnp.broadcast_to(place[:, None], (rows, HD)).astype(jnp.bfloat16)
    payload = jnp.concatenate([queries[0, 0], place], axis=1)
    late_start = planes - 3
    late = order >= late_start
    even = order % 2 == 0
    minus = jnp.where(late, order - late_start + late_start // 2, order // 2)
    evens = (late_start + 1) // 2
    groups = [
        (across == 0, order, planes, 0),
        (across == 1, order, planes, 1),
        (across == 3, order, planes, -1),
        ((across == 2) & even & ~late, order // 2, evens, 2),
        ((across == 2) & (late | ~even), minus, planes - evens, -2),
    ]
    arrived = []
    spot_early, spot_late = jnp.full((rows,), -1, jnp.int32), jnp.full((rows,), -1, jnp.int32)
    base_early, base_late = 0, 0
    for number, (chosen, at, count, by) in enumerate(groups):
        slot = jnp.arange(count * slots, dtype=jnp.int32)[:, None]
        select = (((at * slots + within)[None, :] == slot) & chosen[None, :]).astype(jnp.bfloat16)
        sending = pick(select, payload)
        arrived.append(along_y(sending, by) if by else sending)
        spot_early = jnp.where(chosen & ~late, base_early + at * slots + within, spot_early)
        base_early += slots * (late_start if number < 3 else (evens if number == 3 else late_start // 2))
        if number != 3:
            at_late = base_late + (order - late_start) * slots + within
            spot_late = jnp.where(chosen & late, at_late, spot_late)
            base_late += slots * 3
    select_early = (spot_early[:, None] == jnp.arange(base_early)[None, :]).astype(jnp.bfloat16)
    select_late = (spot_late[:, None] == jnp.arange(base_late)[None, :]).astype(jnp.bfloat16)

    windows = [(window,)]
    ahead_window, behind_window = window, window
    width = window.shape[1] // 2
    for _ in range(1, reach):
        ahead_window = along_z(ahead_window, -1)
        behind_window = along_z(behind_window, 1)
        windows += [(ahead_window,), (behind_window,)]
    last_left = along_z(ahead_window[:, :width], -1)
    last_right = along_z(behind_window[:, width:], 1)
    windows.append((last_left, last_right))

    def serve(orders, batch, buffers):
        return attend(arrived, [windows[order] for order in orders], orders, batch, buffers)

    def give_back(buffers):
        backs = []
        for number, (_, _, _, by) in enumerate(groups):
            if number in buffers:
                backs.append(along_y(buffers[number], -by) if by else buffers[number])
        return backs

    early_orders, late_orders = list(range(late_start)), list(range(late_start, planes))
    buffers = serve(early_orders[:3], early_orders, {})
    for orders in (early_orders[3:7], early_orders[7:]):
        if orders:
            buffers = serve(orders, early_orders, buffers)
    early_backs = give_back(buffers)
    buffers = serve(late_orders[:2], late_orders, {})
    buffers = serve(late_orders[2:], late_orders, buffers)
    late_backs = give_back(buffers)
    partial = collect(select_early, early_backs, [])
    return collect(select_late, late_backs, [partial])[None, None]


def solution(mesh):
    shape = dict(mesh.shape)
    fine = Mesh(
        mesh.devices.reshape(shape["srv"] // COLS, COLS, shape["blk"] // 2, 2, shape["rep"]),
        ("z", "col", "x", "yh", "rep"),
    )
    srv, blk = ("z", "col"), ("x", "yh")
    placed = (
        P(srv, blk, "rep", None),
        P(srv, blk, "rep"),
        P(srv, blk, "rep"),
        P(srv, blk, "rep"),
        P(srv, blk, "rep"),
        P(srv, "rep"),
    )

    return jax.shard_map(
        on_device,
        mesh=fine,
        in_specs=placed,
        out_specs=P(srv, blk, "rep", None),
        check_vma=False,
    )
```
